32 devices in a mesh: dp: 8 (over z, y), section: 4 (over x, core).
Axes of the slice: x: 2, y: 2, z: 4, core: 2. Of those that a mesh axis runs over, the one named last changes fastest.
Arguments:
- embedded: bfloat16 [8, 8, 16, 1024], P('dp'), may hold values from -6 to 6
- lengths: int32 [8, 8], P('dp'), may hold values from 1 to 16
- counts: int32 [8], P('dp'), may hold values from 4 to 8
- labels: int32 [8, 8], P('dp'), may hold values from 0 to 4
- value_weight: bfloat16 [4, 1024, 1024], P('section', 'dp'), may hold values from -0.1875 to 0.1875
- output_projection_weight: bfloat16 [4, 1024, 1024], P('section', 'dp'), may hold values from -0.1875 to 0.1875
- adapter: float32 [4, 1024, 2, 128], P('section', 'dp'), may hold values from -0.1875 to 0.1875
- moment1: float32 [4, 1024, 2, 128], P('section', 'dp'), may hold values from -0.06 to 0.06
- moment2: float32 [4, 1024, 2, 128], P('section', 'dp'), may hold values from 1e-05 to 0.001
- gain: float32 [4, 1024], P('section'), may hold values from 0.25 to 1.75
- position_bias: float32 [4, 16, 16, 16], P('section'), as said below
- head: float32 [1024], replicated, may hold values from -0.1875 to 0.1875
Outputs:
- new_moment1: float32 [4, 1024, 2, 128], P('section', 'dp')
- new_moment2: float32 [4, 1024, 2, 128], P('section', 'dp')
- update: float32 [4, 1024, 2, 128], P('section', 'dp')
The draws below stay inside these ranges and needn't reach their ends.
Inputs may be any that keep to these rules, and one draw needn't show every extreme that they name: `counts`: passages of a query group that take part; those at positions counts and beyond are padding. `lengths`: tokens of a passage that are not padding, the first ones. `position_bias`: real logits.
All inputs are finite; a program needn't handle non-finite values.
Results may differ from the reference program's by a relative error of at most 0.018.
Values may be sent and summed in bfloat16 or wider, within the bound.
No kernel may reach another device: no remote copies, remote signals or barrier semaphores. Data moves between devices by JAX's collectives and lax.ppermute only.
A program may use at most 64 MiB of HBM per device.

```python
import math
import jax
import jax.numpy as jnp
from jax import lax

D = 1024
HEADS = 16
RANK = 128
L = 16
PASS = 8
HD = 1024
GROUPS = 8
N_SECTION = 4


def draw_position_bias(key, part):
    key_base = jax.random.fold_in(key, 0)
    shape = (N_SECTION, HEADS, L, L)
    base = 2.0 * jax.random.normal(key_base, shape, jnp.float32)
    return base


def touch_ends(result, own_key, smallest, high):
    dims = result.shape
    index_at = [jax.random.randint(jax.random.fold_in(own_key, axis), (), 0, dims[axis]) for axis in range(len(dims))]
    result = result.at[tuple(index_at)].set(smallest)
    longest = dims.index(max(dims))
    index_at[longest] = (index_at[longest] + 1) % dims[longest]
    return result.at[tuple(index_at)].set(high)


def block_levels(own_key, dims, shards, smallest, largest):
    loudness, own = 1.0, jax.random.fold_in(own_key, 6)
    for axis_at, shards_of in shards:
        steps = jnp.exp(jax.random.uniform(jax.random.fold_in(own, axis_at), (shards_of,), jnp.float32, smallest / len(shards), largest / len(shards)))
        loudness = loudness * jnp.repeat(steps, dims[axis_at] // shards_of).reshape([-1 if axis == axis_at else 1 for axis in range(len(dims))])
    return loudness


def noise(stream_key, extent, scale, limit, cuts=(), held_as=jnp.bfloat16):
    level = block_levels(stream_key, extent, cuts, -0.22, 0.18) if cuts else 1.0
    result = jax.random.normal(stream_key, extent, jnp.float32) * scale * level
    return jnp.minimum(jnp.maximum(result, -limit), limit).astype(held_as)


def setup_inputs(seed: int = 0) -> dict:
    arg_keys = jax.random.split(jax.random.key(seed), 13)
    embedded = noise(arg_keys[0], (GROUPS, PASS, L, D), 1.0, 6.0, ((0, 8),))
    lengths = touch_ends(jax.random.randint(arg_keys[1], (GROUPS, PASS), 1, L + 1), jax.random.fold_in(arg_keys[1], 1), 1, L).astype(jnp.int32)
    counts = touch_ends(jax.random.randint(arg_keys[2], (GROUPS,), PASS // 2, PASS + 1), jax.random.fold_in(arg_keys[2], 1), PASS // 2, PASS).astype(jnp.int32)
    labels = touch_ends(jax.random.randint(arg_keys[3], (GROUPS, PASS), 0, 5), jax.random.fold_in(arg_keys[3], 1), 0, 4).astype(jnp.int32)
    value_weight = noise(arg_keys[4], (N_SECTION, D, HD), D ** -0.5, 0.1875, ((0, 4), (1, 8)))
    output_projection_weight = noise(arg_keys[5], (N_SECTION, D, HD), HD ** -0.5, 0.1875, ((0, 4), (1, 8)))
    adapter = noise(arg_keys[6], (N_SECTION, D, 2, RANK), D ** -0.5, 0.1875, ((0, 4), (1, 8)), jnp.float32)
    moment1 = noise(arg_keys[7], (N_SECTION, D, 2, RANK), 0.01, 0.06, ((0, 4), (1, 8)), jnp.float32)
    moment2 = jnp.clip(jnp.exp(math.log(0.001) - 4.6051703 * jax.random.uniform(arg_keys[8], (N_SECTION, D, 2, RANK), jnp.float32) ** block_levels(arg_keys[8], (N_SECTION, D, 2, RANK), ((0, 4), (1, 8)), -0.2, 0.2)), 9.999999747378752e-06, 0.001)
    gain = jnp.clip(1.0 + 0.15 * jax.random.normal(arg_keys[9], (N_SECTION, D), jnp.float32), 0.25, 1.75)
    position_bias = draw_position_bias(jax.random.fold_in(arg_keys[12], 71), 0)
    head = noise(arg_keys[11], (D,), D ** -0.5, 0.1875, (), jnp.float32)
    return dict(embedded=embedded, lengths=lengths, counts=counts, labels=labels, value_weight=value_weight, output_projection_weight=output_projection_weight, adapter=adapter, moment1=moment1, moment2=moment2, gain=gain, position_bias=position_bias, head=head)


def probabilities(bias, lens):
    seqlen = bias.shape[-1]
    valid = jnp.arange(seqlen, dtype=jnp.int32)[None, :] < lens[:, None]
    logits = jnp.where(valid[:, None, None, :], bias[None], -1e+30)
    top = lax.optimization_barrier(jnp.max(logits, axis=-1, keepdims=True))
    expo = jnp.exp(logits - top)
    return (expo / lax.optimization_barrier(jnp.sum(expo, axis=-1, keepdims=True))).astype(jnp.bfloat16)

def section_forward(x, lens, wv, wo, adapt, g, bias):
    passages = lens.shape[0]
    heads = bias.shape[0]
    input_flat = x.astype(jnp.float32)
    inverse_scale = jnp.sqrt(lax.optimization_barrier(jnp.mean(input_flat * input_flat, axis=-1, keepdims=True)) + 1e-06)
    normed = (input_flat / inverse_scale * g).astype(jnp.bfloat16)
    value = jnp.dot(normed, wv, preferred_element_type=jnp.float32).astype(jnp.bfloat16)
    probs = probabilities(bias, lens)
    value4 = value.reshape(passages, -1, heads, value.shape[1] // heads)
    attn = jnp.einsum('phij,pjhs->pihs', probs.astype(jnp.float32), value4.astype(jnp.float32), precision=lax.Precision.HIGHEST)
    attn = attn.astype(jnp.bfloat16).reshape(x.shape[0], -1)
    outer = jnp.dot(attn, wo.T, preferred_element_type=jnp.float32)
    latent = jnp.dot(normed, adapt[:, 0], preferred_element_type=jnp.float32).astype(jnp.bfloat16)
    adapted = jnp.dot(latent, adapt[:, 1].T, preferred_element_type=jnp.float32)
    return ((input_flat + outer + adapted).astype(jnp.bfloat16), normed, latent, probs)

def section_backward(grad_out, x, normed, latent, probs, wv, wo, adapt, g):
    passages, heads = (probs.shape[0], probs.shape[1])
    output_gradient_flat = grad_out.astype(jnp.float32)
    dattn = jnp.dot(grad_out, wo, preferred_element_type=jnp.float32).astype(jnp.bfloat16)
    d4 = dattn.reshape(passages, -1, heads, dattn.shape[1] // heads)
    dvalue = jnp.einsum('phij,pihs->pjhs', probs.astype(jnp.float32), d4.astype(jnp.float32), precision=lax.Precision.HIGHEST)
    dvalue = dvalue.astype(jnp.bfloat16).reshape(x.shape[0], -1)
    dlatent = jnp.dot(grad_out, adapt[:, 1], preferred_element_type=jnp.float32).astype(jnp.bfloat16)
    da = jnp.dot(dvalue, wv.T, preferred_element_type=jnp.float32) + jnp.dot(dlatent, adapt[:, 0].T, preferred_element_type=jnp.float32)
    input_flat = x.astype(jnp.float32)
    inverse_scale = jnp.sqrt(lax.optimization_barrier(jnp.mean(input_flat * input_flat, axis=-1, keepdims=True)) + 1e-06)
    input_standardized = input_flat / inverse_scale
    norm_gradient = da * g
    input_gradient = output_gradient_flat + (norm_gradient - input_standardized * lax.optimization_barrier(jnp.mean(norm_gradient * input_standardized, axis=-1, keepdims=True))) / inverse_scale
    term_down = jnp.dot(normed.T, dlatent, preferred_element_type=jnp.float32)
    term_up = jnp.dot(grad_out.T, latent, preferred_element_type=jnp.float32)
    return (input_gradient.astype(jnp.bfloat16), jnp.stack([term_down, term_up], axis=1))

def group_loss(scores, lab, count):
    idx = jnp.arange(lab.shape[0], dtype=jnp.int32)
    valid = idx < count
    left = lab[:, None]
    right = lab[None, :]
    before = ((right > left) | (right == left) & (idx[None, :] < idx[:, None])) & valid[None, :]
    rank = lax.optimization_barrier(jnp.sum(before.astype(jnp.int32), axis=1))
    gains = jnp.exp2(lab.astype(jnp.float32)) - 1.0
    disc = 1.0 / jnp.log2(2.0 + rank.astype(jnp.float32))
    pair = (left > right) & valid[:, None] & valid[None, :]
    weights = jnp.where(pair, jnp.abs(gains[:, None] - gains[None, :]) * jnp.abs(disc[:, None] - disc[None, :]), 0.0)
    ideal = jnp.sum(jnp.where(valid, gains * disc, 0.0))
    margin = scores[:, None] - scores[None, :]
    return jnp.sum(weights * jax.nn.softplus(-margin)) / jnp.maximum(ideal, 1.0)

def loss_cotangent(final, lens, count, lab, head):
    tokens = final.shape[1]
    mask = (jnp.arange(tokens, dtype=jnp.int32)[None, :] < lens[:, None]).astype(jnp.float32)
    pooled = jnp.einsum('pt,ptd->pd', mask, final.astype(jnp.float32), precision=lax.Precision.HIGHEST)
    denom = lens.astype(jnp.float32)
    scores = jnp.dot(pooled / denom[:, None], head, precision=lax.Precision.HIGHEST)
    dscore = jax.grad(group_loss)(scores, lab, count)
    cot = dscore[:, None, None] * head[None, None, :] * mask[:, :, None] / denom[:, None, None]
    return cot.astype(jnp.bfloat16)

def reference(embedded, lengths, counts, labels, value_weight, output_projection_weight, adapter, moment1, moment2, gain, position_bias, head):
    sections = value_weight.shape[0]
    width = value_weight.shape[1]
    adapt_b = adapter.astype(jnp.bfloat16)

    def one_group(total, item):
        emb, lens, count, lab = item
        x = emb.reshape(-1, width)
        saved = []
        for s in range(sections):
            y, normed, latent, probs = section_forward(x, lens, value_weight[s], output_projection_weight[s], adapt_b[s], gain[s], position_bias[s])
            saved.append((x, normed, latent, probs))
            x = y
        grad_out = loss_cotangent(x.reshape(emb.shape), lens, count, lab, head).reshape(x.shape)
        terms = [None] * sections
        for s in reversed(range(sections)):
            xs, normed, latent, probs = saved[s]
            grad_out, term = section_backward(grad_out, xs, normed, latent, probs, value_weight[s], output_projection_weight[s], adapt_b[s], gain[s])
            terms[s] = term
        return (total + jnp.stack(terms), None)
    start = jnp.zeros(adapter.shape, jnp.float32)
    grad, _ = lax.scan(one_group, start, (embedded, lengths, counts, labels))
    new_moment1 = 0.9 * moment1 + 0.1 * grad
    new_moment2 = 0.999 * moment2 + 0.001 * grad * grad
    update = new_moment1 / (1.0 - 0.9 ** 10) / (jnp.sqrt(new_moment2 / (1.0 - 0.999 ** 10)) + 1e-08)
    return (new_moment1, new_moment2, update)
```

```python
import functools

import jax
import jax.numpy as jnp
from jax import lax
from jax.experimental import pallas as pl
from jax.experimental.pallas import tpu as pltpu
from jax.sharding import PartitionSpec as P


F32 = jnp.float32
BF16 = jnp.bfloat16
LANES = 128
NN = (((1,), (0,)), ((), ()))
NT = (((1,), (1,)), ((), ()))
TN = (((0,), (0,)), ((), ()))
VMEM = pl.BlockSpec(memory_space=pltpu.VMEM)
SMEM = pl.BlockSpec(memory_space=pltpu.SMEM)
ANY = pl.BlockSpec(memory_space=pl.ANY)


def limit(mib):
    return pltpu.CompilerParams(vmem_limit_bytes=mib * 1024 * 1024)


def dot(a, b, dims=NN):
    return lax.dot_general(a, b, dims, preferred_element_type=F32)


def step_of(width):
    return 256 if width % 256 == 0 else width


def dp_index():
    return lax.axis_index("dp")


def pack_kernel(out_ref, adapter_ref, joined_ref):
    wide = out_ref.shape[1]
    rank = adapter_ref.shape[2]
    joined_ref[:, :wide] = out_ref[...]
    for k in range(adapter_ref.shape[1]):
        at = wide + k * rank
        joined_ref[:, at : at + rank] = adapter_ref[:, k, :].astype(BF16)


def assemble_kernel(sources, size, *refs):
    outer, inner = split(size)
    arrays = refs[: len(sources)]
    whole, sems = refs[-2:]
    index = dp_index()
    copies = []
    for at, (far, near) in enumerate(sources):
        rows = arrays[at].shape[0]
        z = (index // inner + far + outer) % outer
        y = (index + near) % inner
        begin = pl.multiple_of((z * inner + y) * rows, rows)
        copies.append(pltpu.make_async_copy(arrays[at], whole.at[pl.ds(begin, rows)], sems.at[at]))
    for copy in copies:
        copy.start()
    for copy in copies:
        copy.wait()


def assemble(arrays, sources, size, earlier=None):
    count = len(arrays)
    rows, columns = arrays[0].shape
    more = [] if earlier is None else [earlier]
    return pl.pallas_call(
        functools.partial(assemble_kernel, sources, size),
        out_shape=jax.ShapeDtypeStruct((rows * size, columns), arrays[0].dtype),
        in_specs=[VMEM] * (count + len(more)),
        out_specs=VMEM,
        scratch_shapes=[pltpu.SemaphoreType.DMA((count,))],
        input_output_aliases={count: 0} if more else {},
        compiler_params=limit(8),
        name="assemble",
    )(*arrays, *more)


def transposed(row, eye):
    return jnp.sum(jnp.where(eye, row, 0.0), axis=1, keepdims=True)


def pair_kernel(lens_ref, counts_ref, labels_ref, lengths_ref, pool_ref, poolt_ref, pair_ref, pairt_ref, lenc_ref, lenr_ref):
    groups, count, rows = pool_ref.shape
    seqlen = rows // count
    across = lax.broadcasted_iota(jnp.int32, (count, count), 1)
    along = lax.broadcasted_iota(jnp.int32, (count, count), 0)
    eye = across == along
    for g in range(groups):
        valid_row = across < counts_ref[g]
        valid_col = along < counts_ref[g]
        row = jnp.broadcast_to(labels_ref[g : g + 1, :].astype(F32), (count, count))
        col = jnp.broadcast_to(transposed(row, eye), (count, count))
        ahead = ((col > row) | (col == row) & (along < across)) & valid_col
        disc_row = 1.0 / jnp.log2(2.0 + jnp.sum(ahead.astype(F32), axis=0, keepdims=True))
        ahead = ((row > col) | (row == col) & (across < along)) & valid_row
        disc_col = 1.0 / jnp.log2(2.0 + jnp.sum(ahead.astype(F32), axis=1, keepdims=True))
        gain_row = jnp.exp2(row) - 1.0
        gain_col = jnp.exp2(col) - 1.0
        once = jnp.where(valid_row & (along == 0), gain_row * disc_row, 0.0)
        ideal = jnp.maximum(jnp.sum(jnp.sum(once, axis=1, keepdims=True), axis=0, keepdims=True), 1.0)
        gap = jnp.abs(gain_row - gain_col) * jnp.abs(disc_row - disc_col) / ideal
        valid = valid_row & valid_col
        pair_ref[g] = jnp.where(valid & (col > row), gap, 0.0)
        pairt_ref[g] = jnp.where(valid & (row > col), gap, 0.0)
        lens = lengths_ref[g : g + 1, :].astype(F32)
        lenr_ref[g] = lens
        lenc_ref[g] = transposed(jnp.broadcast_to(lens, (count, count)), eye)
        lane = lax.broadcasted_iota(jnp.int32, (count, rows), 1)
        passage = lax.broadcasted_iota(jnp.int32, (count, rows), 0)
        held = lane % seqlen < lenc_ref[g].astype(jnp.int32)
        pool_ref[g] = ((lane // seqlen == passage) & held).astype(F32).astype(BF16)
        place = lax.broadcasted_iota(jnp.int32, (rows, count), 0)
        passage = lax.broadcasted_iota(jnp.int32, (rows, count), 1)
        held = place % seqlen < lengths_ref[g : g + 1, :]
        poolt_ref[g] = ((place // seqlen == passage) & held).astype(F32)


def prob_kernel(lens_ref, bias_ref, probs_ref, probst_ref):
    heads, seqlen, _ = bias_ref.shape
    groups, _, rows, _ = probs_ref.shape
    passages = rows // seqlen
    spread = lax.broadcasted_iota(jnp.int32, (seqlen, rows), 1) % seqlen
    spread = (spread == lax.broadcasted_iota(jnp.int32, (seqlen, rows), 0)).astype(F32)
    tiled = lax.dot_general(
        bias_ref[...].reshape(heads * seqlen, seqlen),
        spread,
        NN,
        precision=lax.Precision.HIGHEST,
        preferred_element_type=F32,
    )
    lane = lax.broadcasted_iota(jnp.int32, (rows, rows), 1)
    same = lane // seqlen == lax.broadcasted_iota(jnp.int32, (rows, rows), 0) // seqlen
    for g in range(groups):
        held = [jnp.full((seqlen, rows), lens_ref[g, p], jnp.int32) for p in range(passages)]
        mask = same & (lane % seqlen < jnp.concatenate(held, axis=0))
        for h in range(heads):
            block = tiled[h * seqlen : (h + 1) * seqlen]
            logits = jnp.where(mask, jnp.concatenate([block] * passages, axis=0), -1e30)
            expo = jnp.exp(logits - jnp.max(logits, axis=-1, keepdims=True))
            prob = expo / jnp.sum(expo, axis=-1, keepdims=True)
            probs_ref[g, h] = prob.astype(BF16)
            probst_ref[g, h] = prob.T.astype(BF16)


def normalize(x_ref):
    x = x_ref[...].astype(F32)
    r = jnp.sqrt(jnp.mean(x * x, axis=-1, keepdims=True) + 1e-06)
    return x, r


def mix_heads(prob_ref, src_ref, dst_ref, groups, head_width):
    rows = prob_ref.shape[2]
    width = src_ref.shape[1]
    per = max(1, LANES // head_width)
    span = per * head_width
    lane = lax.broadcasted_iota(jnp.int32, (rows, span), 1) // head_width
    for g in range(groups):
        at = pl.ds(g * rows, rows)
        for b in range(width // span):
            cols = pl.ds(b * span, span)
            block = src_ref[at, cols]
            if per == 1:
                mixed = dot(prob_ref[g, b], block)
            else:
                zero = jnp.zeros_like(block)
                stack = jnp.concatenate([jnp.where(lane == i, block, zero) for i in range(per)], axis=0)
                probs = jnp.concatenate([prob_ref[g, b * per + i] for i in range(per)], axis=1)
                mixed = dot(probs, stack)
            dst_ref[at, cols] = mixed.astype(BF16)


def forward_body(x_ref, gain_ref, prob_ref, y_ref, norm_ref, z_ref, wv, wb, value, attn, cfg):
    groups, head_width, width, hd, rank = cfg
    x, r = normalize(x_ref)
    norm_ref[...] = (x / r * gain_ref[...]).astype(BF16)
    step = step_of(hd)
    for c in range(0, hd, step):
        value[:, c : c + step] = dot(norm_ref[...], wv[:, c : c + step]).astype(BF16)
    mix_heads(prob_ref, value, attn, groups, head_width)
    z = dot(norm_ref[...], wb[:, hd : hd + rank]).astype(BF16)
    z_ref[...] = z
    step = step_of(width)
    for c in range(0, width, step):
        out = dot(attn[...], wb[c : c + step, :hd], NT)
        adapted = dot(z, wb[c : c + step, hd + rank :], NT)
        y_ref[:, c : c + step] = (x_ref[:, c : c + step].astype(F32) + out + adapted).astype(BF16)


def backward_body(dy_ref, x_ref, gain_ref, probt_ref, dx_ref, dz_ref, wv, wb, value, attn, cfg):
    groups, head_width, width, hd, rank = cfg
    step = step_of(hd)
    for c in range(0, hd, step):
        value[:, c : c + step] = dot(dy_ref[...], wb[:, c : c + step]).astype(BF16)
    dz_ref[...] = dot(dy_ref[...], wb[:, hd + rank :]).astype(BF16)
    mix_heads(probt_ref, value, attn, groups, head_width)
    step = step_of(width)
    x, r = normalize(x_ref)
    xhat = x / r
    parts = []
    total = jnp.zeros((x.shape[0], 1), F32)
    for c in range(0, width, step):
        da = dot(attn[...], wv[c : c + step, :], NT)
        da = da + dot(dz_ref[...], wb[c : c + step, hd : hd + rank], NT)
        dn = da * gain_ref[:, c : c + step]
        parts.append(dn)
        total = total + jnp.sum(dn * xhat[:, c : c + step], axis=-1, keepdims=True)
    mean = total / width
    for at, c in enumerate(range(0, width, step)):
        dx = (parts[at] - xhat[:, c : c + step] * mean) / r
        dx_ref[:, c : c + step] = (dy_ref[:, c : c + step].astype(F32) + dx).astype(BF16)


def grad_body(norm_ref, z_ref, dy_ref, dz_ref, grad_ref, outs, cfg):
    _, _, width, _, rank = cfg
    target = grad_ref if len(outs) > 1 else outs[0]
    step = step_of(width)
    for c in range(0, width, step):
        target[c : c + step, :rank] = dot(norm_ref[:, c : c + step], dz_ref[...], TN).astype(BF16)
        target[c : c + step, rank:] = dot(dy_ref[:, c : c + step], z_ref[...], TN).astype(BF16)
    if len(outs) > 1:
        rows = width // len(outs)
        for k, out in enumerate(outs):
            begin = pl.multiple_of((dp_index() ^ k) * rows, rows)
            out[...] = grad_ref[pl.ds(begin, rows), :]


def loss_body(y_ref, head_ref, pool_ref, poolt_ref, pair_ref, pairt_ref, lenc_ref, lenr_ref, dy_ref, groups):
    rows = pool_ref.shape[2]
    count = pool_ref.shape[1]
    eye = lax.broadcasted_iota(jnp.int32, (count, count), 0) == lax.broadcasted_iota(
        jnp.int32, (count, count), 1
    )
    for g in range(groups):
        at = pl.ds(g * rows, rows)
        pooled = dot(pool_ref[g], y_ref[at, :])
        column = jnp.sum(pooled / lenc_ref[g] * head_ref[...], axis=-1, keepdims=True)
        line = jnp.sum(jnp.where(eye, column, 0.0), axis=0, keepdims=True)
        up = pair_ref[g] * jax.nn.sigmoid(line - column)
        down = pairt_ref[g] * jax.nn.sigmoid(column - line)
        dscore = jnp.sum(up - down, axis=0, keepdims=True)
        scale = jnp.sum(poolt_ref[g] * (dscore / lenr_ref[g]), axis=-1, keepdims=True)
        dy_ref[at, :] = (scale * head_ref[...]).astype(BF16)


def forward_kernel(tick, cfg, *refs):
    x_ref, gain_ref, prob_ref, wv, wb, y_ref, norm_ref, z_ref, value, attn = refs

    @pl.when(lax.axis_index("section") == tick)
    def _():
        forward_body(x_ref, gain_ref, prob_ref, y_ref, norm_ref, z_ref, wv, wb, value, attn, cfg)


def middle_kernel(tick, pieces, cfg, *refs):
    x_ref, gain_ref, prob_ref, probt_ref, wv, wb = refs[:6]
    loss_refs = refs[6:13]
    dx_ref = refs[13]
    outs = refs[14 : 14 + pieces]
    value, attn, y_ref, norm_ref, z_ref, dy_ref, dz_ref, grad_ref = refs[14 + pieces :]

    @pl.when(lax.axis_index("section") == tick)
    def _():
        forward_body(x_ref, gain_ref, prob_ref, y_ref, norm_ref, z_ref, wv, wb, value, attn, cfg)
        loss_body(y_ref, *loss_refs, dy_ref, cfg[0])
        backward_body(dy_ref, x_ref, gain_ref, probt_ref, dx_ref, dz_ref, wv, wb, value, attn, cfg)
        grad_body(norm_ref, z_ref, dy_ref, dz_ref, grad_ref, outs, cfg)


def backward_kernel(tick, pieces, cfg, *refs):
    dy_ref, x_ref, gain_ref, probt_ref, wv, wb, norm_ref, z_ref = refs[:8]
    dx_ref = refs[8 + pieces]
    outs = refs[9 + pieces : 9 + 2 * pieces]
    value, attn, dz_ref, grad_ref = refs[9 + 2 * pieces :]

    @pl.when(lax.axis_index("section") == tick)
    def _():
        backward_body(dy_ref, x_ref, gain_ref, probt_ref, dx_ref, dz_ref, wv, wb, value, attn, cfg)
        grad_body(norm_ref, z_ref, dy_ref, dz_ref, grad_ref, outs, cfg)


def first_kernel(tick, pieces, cfg, *refs):
    dy_ref, wb, norm_ref, z_ref = refs[:4]
    outs = refs[4 : 4 + pieces]
    dz_ref, grad_ref = refs[4 + pieces :]
    hd, rank = cfg[3], cfg[4]

    @pl.when(lax.axis_index("section") == tick)
    def _():
        dz_ref[...] = dot(dy_ref[...], wb[:, hd + rank :]).astype(BF16)
        grad_body(norm_ref, z_ref, dy_ref, dz_ref, grad_ref, outs, cfg)


def adam_kernel(each, *refs):
    parts = refs[: 2 * each]
    m1_ref, m2_ref, new1_ref, new2_ref, update_ref, grad_ref = refs[2 * each :]
    first = lax.axis_index("section") == 0
    for s, here in enumerate((first, jnp.logical_not(first))):

        @pl.when(here)
        def _(s=s):
            grad = parts[s * each][...].astype(F32)
            for part in parts[s * each + 1 : (s + 1) * each]:
                grad = grad + part[...].astype(F32)
            grad_ref[...] = grad

    rank = m1_ref.shape[2]
    for k in range(m1_ref.shape[1]):
        slab = grad_ref[:, k * rank : (k + 1) * rank]
        new1 = 0.9 * m1_ref[:, k, :] + 0.1 * slab
        new2 = 0.999 * m2_ref[:, k, :] + 0.001 * slab * slab
        new1_ref[:, k, :] = new1
        new2_ref[:, k, :] = new2
        update_ref[:, k, :] = new1 / (1.0 - 0.9**10) / (jnp.sqrt(new2 / (1.0 - 0.999**10)) + 1e-08)


def split(size):
    inner = 2 if size % 2 == 0 else 1
    return size // inner, inner


def by_neighbours(size):
    return split(size)[0] <= 4


def by_pairs(size):
    return size <= 8 and size & (size - 1) == 0


def turns(outer):
    steps = []
    for k in range(1, outer // 2 + 1):
        steps.append((-1, k))
        if 2 * k < outer:
            steps.append((1, k))
    return steps


def spread(chunks, size):
    outer, inner = split(size)
    if not by_neighbours(size):
        return [lax.all_gather(chunk, "dp", axis=0, tiled=True) for chunk in chunks]

    def swapped(array):
        pairs = [(z * inner + y, z * inner + (y + 1) % inner) for z in range(outer) for y in range(inner)]
        return lax.ppermute(array, "dp", pairs)

    wholes = []
    for chunk in chunks:
        held = {0: chunk}
        for side, k in turns(outer):
            pairs = [(z * inner + y, (z - side) % outer * inner + y) for z in range(outer) for y in range(inner)]
            held[side * k] = lax.ppermute(held[side * (k - 1)], "dp", pairs)
        order = [0] + [side * k for side, k in turns(outer)]
        arrays, sources = [], []
        for far in order:
            arrays.append(held[far])
            sources.append((far, 0))
            if inner == 2:
                arrays.append(swapped(held[far]))
                sources.append((far, 1))
        cutoff = len(arrays) - inner if outer > 1 else len(arrays)
        whole = assemble(arrays[:cutoff], tuple(sources[:cutoff]), size)
        if cutoff < len(arrays):
            whole = assemble(arrays[cutoff:], tuple(sources[cutoff:]), size, whole)
        wholes.append(whole)
    return wholes


def exchange(pieces, size, sections, due):
    parts = [pieces[0]]
    for k in range(1, size):
        pairs = [(i * sections + s, (i ^ k) * sections + s) for i in range(size) for s in due]
        parts.append(lax.ppermute(pieces[k], ("dp", "section"), pairs))
    return parts


def shards(
    embedded,
    lengths,
    counts,
    labels,
    value_weight,
    output_projection_weight,
    adapter,
    moment1,
    moment2,
    gain,
    position_bias,
    head,
):
    size = lax.axis_size("dp")
    sections = lax.axis_size("section")
    section = lax.axis_index("section")
    groups, passages, seqlen, width = embedded.shape
    rows = passages * seqlen
    total = groups * rows
    hd = value_weight.shape[2]
    heads = position_bias.shape[1]
    rank = adapter.shape[3]
    cfg = (groups, hd // heads, width, hd, rank)
    own = value_weight.shape[1]

    joined = pl.pallas_call(
        pack_kernel,
        out_shape=jax.ShapeDtypeStruct((own, hd + 2 * rank), BF16),
        in_specs=[VMEM, VMEM],
        out_specs=VMEM,
        compiler_params=limit(4),
        name="pack",
    )(output_projection_weight[0], adapter[0])
    wv, wb = spread([value_weight[0], joined], size)

    square = jax.ShapeDtypeStruct((groups, heads, rows, rows), BF16)
    probs, probst = pl.pallas_call(
        prob_kernel,
        out_shape=(square, square),
        in_specs=[SMEM, VMEM],
        out_specs=(VMEM, VMEM),
        compiler_params=limit(8),
        name="prob",
    )(lengths, position_bias[0])
    shapes = [(passages, rows), (rows, passages), (passages, passages), (passages, passages), (passages, 1), (1, passages)]
    types = [BF16] + [F32] * 5
    loss_in = pl.pallas_call(
        pair_kernel,
        out_shape=tuple(jax.ShapeDtypeStruct((groups,) + a, b) for a, b in zip(shapes, types)),
        in_specs=[SMEM, SMEM, VMEM, VMEM],
        out_specs=(VMEM,) * 6,
        compiler_params=limit(4),
        name="pair",
    )(lengths, counts, labels, lengths)
    loss_in = (head[None, :],) + tuple(loss_in)

    pieces = size if by_pairs(size) else 1
    act = jax.ShapeDtypeStruct((total, width), BF16)
    low_act = jax.ShapeDtypeStruct((total, rank), BF16)
    grads = (jax.ShapeDtypeStruct((width // pieces, 2 * rank), BF16),) * pieces
    mixed = [pltpu.VMEM((total, hd), BF16)] * 2
    wide = pltpu.VMEM((total, width), BF16)
    thin = pltpu.VMEM((total, rank), BF16)
    gbuf = pltpu.VMEM((width, 2 * rank), BF16)

    x = embedded.reshape(total, width)
    saved = []
    for tick in range(sections - 1):
        y, normed, z = pl.pallas_call(
            functools.partial(forward_kernel, tick, cfg),
            out_shape=(act, act, low_act),
            in_specs=[VMEM] * 5,
            out_specs=(VMEM,) * 3,
            scratch_shapes=mixed,
            compiler_params=limit(12),
        )(x, gain, probs, wv, wb)
        saved.append((x, normed, z))
        x = lax.ppermute(y, "section", [(tick, tick + 1)])
    last = sections - 1
    dx, *grad = pl.pallas_call(
        functools.partial(middle_kernel, last, pieces, cfg),
        out_shape=(act,) + grads,
        in_specs=[VMEM] * 13,
        out_specs=(VMEM,) * (1 + pieces),
        scratch_shapes=mixed + [wide, wide, thin, wide, thin, gbuf],
        compiler_params=limit(14),
        name="middle",
    )(x, gain, probs, probst, wv, wb, *loss_in)
    later = grad
    for tick in range(last - 1, 0, -1):
        dy = lax.ppermute(dx, "section", [(tick + 1, tick)])
        x, normed, z = saved[tick]
        dx, *grad = pl.pallas_call(
            functools.partial(backward_kernel, tick, pieces, cfg),
            out_shape=(act,) + grads,
            in_specs=[VMEM] * (8 + pieces),
            input_output_aliases={8 + i: 1 + i for i in range(pieces)},
            out_specs=(VMEM,) * (1 + pieces),
            scratch_shapes=mixed + [thin, gbuf],
            compiler_params=limit(13),
        )(dy, x, gain, probst, wv, wb, normed, z, *later)
        later = grad
    if last > 0:
        dy = lax.ppermute(dx, "section", [(1, 0)])
        _, normed, z = saved[0]
        early = pl.pallas_call(
            functools.partial(first_kernel, 0, pieces, cfg),
            out_shape=grads,
            in_specs=[VMEM] * 4,
            out_specs=(VMEM,) * pieces,
            scratch_shapes=[thin, gbuf],
            compiler_params=limit(8),
            name="first",
        )(dy, wb, normed, z)
    else:
        early = later
    if by_pairs(size):
        parts = exchange(early, size, sections, (0,))
        parts += exchange(later, size, sections, range(1, sections))
    else:
        held = jnp.where(section == 0, early[0], later[0]).astype(F32)
        parts = [lax.psum_scatter(held, "dp", scatter_dimension=0, tiled=True)] * 2
    state = jax.ShapeDtypeStruct(moment1.shape[1:], F32)
    outs = pl.pallas_call(
        functools.partial(adam_kernel, len(parts) // 2),
        out_shape=(state, state, state),
        in_specs=[VMEM] * (len(parts) + 2),
        out_specs=(VMEM,) * 3,
        scratch_shapes=[pltpu.VMEM((own, 2 * rank), F32)],
        compiler_params=limit(8),
        name="adam",
    )(*parts, moment1[0], moment2[0])
    return tuple(out[None] for out in outs)


def solution(mesh):
    in_specs = (
        P("dp", None, None, None),
        P("dp", None),
        P("dp"),
        P("dp", None),
        P("section", "dp", None),
        P("section", "dp", None),
        P("section", "dp", None, None),
        P("section", "dp", None, None),
        P("section", "dp", None, None),
        P("section", None),
        P("section", None, None, None),
        P(),
    )
    out_specs = (
        P("section", "dp", None, None),
        P("section", "dp", None, None),
        P("section", "dp", None, None),
    )
    return jax.shard_map(shards, mesh=mesh, in_specs=in_specs, out_specs=out_specs, check_vma=False)
```
